16 devices in a mesh: data: 2 (over z), tp: 8 (over y, x, core).
Axes of the slice: x: 2, y: 2, z: 2, core: 2. Of those that a mesh axis runs over, the one named last changes fastest.
Arguments:
- X: bfloat16 [8192, 3072], P(('data', 'tp')), parts along dimension 0
- gamma: float32 [3072], replicated
- W1: bfloat16 [3072, 8192], P(None, 'tp')
- W2: bfloat16 [8192, 3072], P('tp')
- dY: bfloat16 [8192, 3072], P(('data', 'tp')), parts along dimension 0
Outputs:
- output 1: bfloat16 [8192, 3072], P(('data', 'tp')), parts along dimension 0
- output 2: bfloat16 [8192, 3072], P(('data', 'tp')), parts along dimension 0
- output 3: float32 [6144, 8192], P('data', 'tp'), parts along dimension 0
- output 4: float32 [16384, 3072], P(('data', 'tp')), parts along dimension 0
- output 5: float32 [6144], P('data'), parts along dimension 0
There are 2 independent parts. The reference program is written for one: setup_inputs(seed, part) draws one part's arguments, and reference() takes and returns one part's arrays. A program takes and returns all parts, laid end to end along the dimension named above; an argument that names none is the same for every part.
All inputs are finite; a program needn't handle non-finite values.
Results may differ from the reference program's by a relative error of at most 0.001.
Values are sent between devices in bfloat16 or wider.
A program may use at most 1 GiB of HBM per device.

```python
import jax
import jax.numpy as jnp
from jax import lax

S = 4096
D = 3072
F = 8192
EPS = 1e-6


def setup_inputs(seed: int = 0, part: int = 0) -> dict:
    key = jax.random.key(seed)
    kg, k1, k2, kbase = jax.random.split(key, 4)
    kx, ky = jax.random.split(jax.random.fold_in(kbase, part))
    X = jax.random.normal(kx, (S, D), jnp.float32).astype(jnp.bfloat16)
    gamma = 1.0 + 0.2 * jax.random.normal(kg, (D,), jnp.float32)
    W1 = (jax.random.normal(k1, (D, F), jnp.float32) * D ** -0.5).astype(jnp.bfloat16)
    W2 = (jax.random.normal(k2, (F, D), jnp.float32) * (1.5 * F ** -0.5)).astype(jnp.bfloat16)
    dY = jax.random.normal(ky, (S, D), jnp.float32).astype(jnp.bfloat16)
    return {"X": X, "gamma": gamma, "W1": W1, "W2": W2, "dY": dY}


def _gelu(a):
    return jax.nn.gelu(a, approximate=True)


def reference(X, gamma, W1, W2, dY):
    x = X.astype(jnp.float32)
    mu = jnp.mean(x, axis=-1, keepdims=True)
    xc = x - mu
    var = jnp.mean(xc * xc, axis=-1, keepdims=True)
    rstd = lax.rsqrt(var + EPS)
    xhatv = xc * rstd
    Xn = (xhatv * gamma).astype(jnp.bfloat16)
    A = jnp.dot(Xn, W1, preferred_element_type=jnp.float32)
    H = _gelu(A).astype(jnp.bfloat16)
    Y = (x + jnp.dot(H, W2, preferred_element_type=jnp.float32)).astype(jnp.bfloat16)
    dW2 = jnp.dot(H.T, dY, preferred_element_type=jnp.float32)
    dH = jnp.dot(dY, W2.T, preferred_element_type=jnp.float32)
    dA = jax.vjp(_gelu, A)[1](dH)[0].astype(jnp.bfloat16)
    dW1 = jnp.dot(Xn.T, dA, preferred_element_type=jnp.float32)
    dXn = jnp.dot(dA, W1.T, preferred_element_type=jnp.float32)
    dgamma = jnp.sum(dXn * xhatv, axis=0)
    dxhat = dXn * gamma
    dx = rstd * (dxhat - jnp.mean(dxhat, axis=-1, keepdims=True) - xhatv * jnp.mean(dxhat * xhatv, axis=-1, keepdims=True))
    dX = (dY.astype(jnp.float32) + dx).astype(jnp.bfloat16)
    return (Y, dX, dW1, dW2, dgamma)
```

```python
import jax
import jax.numpy as jnp
from jax import lax
from jax.sharding import PartitionSpec as P


EPS = 1e-6
BF = jnp.bfloat16
F32 = jnp.float32


def _gelu(a):
    return jax.nn.gelu(a, approximate=True)


def _ln(x):
    mu = jnp.mean(x, axis=-1, keepdims=True)
    xc = x - mu
    var = jnp.mean(xc * xc, axis=-1, keepdims=True)
    rstd = lax.rsqrt(var + EPS)
    return xc * rstd, rstd


def _nn(a, b):
    return jnp.dot(a, b, preferred_element_type=F32)


def _tn(a, b):
    return lax.dot_general(a, b, (((0,), (0,)), ((), ())), preferred_element_type=F32)


def _nt(a, b):
    return lax.dot_general(a, b, (((1,), (1,)), ((), ())), preferred_element_type=F32)


def _swap(bit):
    return lambda v: lax.ppermute(v, "tp", [(i, i ^ bit) for i in range(8)])


CORE, XN, YN = _swap(1), _swap(2), _swap(4)


def ZN(v):
    return lax.ppermute(v, "data", [(0, 1), (1, 0)])


def _dact(A, dH):
    return jax.vjp(_gelu, A)[1](dH)[0].astype(BF)


def _cat(*v):
    return jnp.concatenate(v)


tie = lambda *v: lax.optimization_barrier(v)


def solution(mesh):
    rows = P(("data", "tp"), None)

    def block(X, gamma, W1, W2, dY):
        n = X.shape[0]
        zi = lax.axis_index("data")
        half = W2.shape[0] // 2
        q = half // 2
        W1T = W1.T

        def piece(w, c):
            return lax.dynamic_slice_in_dim(w, zi * half + c * q, q, 0)

        def group(Xnc, dYc, w1, w2, Yp, dXp):
            Ak = _nt(Xnc, w1)
            Yp = Yp + _nn(_gelu(Ak).astype(BF), w2)
            dXp = dXp + _nn(_dact(Ak, _nt(dYc, w2)), w1)
            return Yp, dXp

        Xp, dYp = CORE(X), CORE(dY)
        a1, a2 = piece(W1T, 0), piece(W2, 0)
        x1, y1, x2, y2 = XN(a1), YN(a1), XN(a2), YN(a2)
        Xs, a1, a2 = tie(X, a1, a2)
        x = Xs.astype(F32)
        xhat, rstd = _ln(x)
        Xn = (xhat * gamma).astype(BF)
        Xa = lax.all_gather(Xn, "tp", axis=0, tiled=True)
        dYs, W1s, W2s, Xn, Xp, dYp = tie(dY, W1T, W2, Xn, Xp, dYp)
        g = lax.all_gather(dYs, "tp", axis=0, tiled=True)
        b1, b2 = piece(W1s, 1), piece(W2s, 1)
        bx1, by1, bx2, by2 = XN(b1), YN(b1), XN(b2), YN(b2)
        b1, b2, Xp = tie(b1, b2, Xp)
        Xnc = _cat(Xn, (_ln(Xp.astype(F32))[0] * gamma).astype(BF))
        dYc = _cat(dY, dYp)

        A0 = _nn(Xnc, W1)
        dA0 = _dact(A0, _nt(dYc, W2))
        x1, y1, A0, dA0 = tie(x1, y1, A0, dA0)
        zx1, zy1, d1 = ZN(x1), ZN(y1), XN(y1)
        P0, Q0 = _nn(_gelu(A0).astype(BF), W2), _nt(dA0, W1)
        x2, y2, P0, Q0 = tie(x2, y2, P0, Q0)
        zx2, zy2, d2 = ZN(x2), ZN(y2), YN(x2)

        Xa, P0, Q0 = tie(Xa, P0, Q0)
        A = _nn(Xa, W1)
        d1, d2, bx1, by1, bx2, by2, A = tie(d1, d2, bx1, by1, bx2, by2, A)
        zd1, zd2 = ZN(d1), ZN(d2)
        bzx1, bzy1, bzx2, bzy2 = ZN(bx1), ZN(by1), ZN(bx2), ZN(by2)
        bd1, bd2 = XN(by1), YN(bx2)
        g, A = tie(g, A)
        dA = _dact(A, _nt(g, W2))
        bd1, bd2, dA, gs = tie(bd1, bd2, dA, g)
        bzd1, bzd2 = ZN(bd1), ZN(bd2)
        dW2 = _tn(_gelu(A).astype(BF), gs)
        zx1, zy1, zx2, zy2, zd1, zd2, dW2 = tie(zx1, zy1, zx2, zy2, zd1, zd2, dW2)
        P1, Q1 = group(Xnc, dYc, _cat(x1, y1, d1, zx1, zy1, zd1), _cat(x2, y2, d2, zx2, zy2, zd2), P0, Q0)
        P1, Q1, dA = tie(P1, Q1, dA)
        dW1 = _tn(Xa, dA)
        bzx1, bzy1, bzx2, bzy2, bzd1, bzd2, dW1 = tie(bzx1, bzy1, bzx2, bzy2, bzd1, bzd2, dW1)
        Yp, dXp = group(Xnc, dYc, _cat(bx1, by1, bd1, bzx1, bzy1, bzd1), _cat(bx2, by2, bd2, bzx2, bzy2, bzd2), P1, Q1)

        dXn = dXp[:n] + CORE(dXp[n:])
        Y = (x + (Yp[:n] + CORE(Yp[n:]))).astype(BF)
        dgamma = jnp.sum(dXn * xhat, axis=0)
        for hop in (CORE, XN, YN):
            dgamma = dgamma + hop(dgamma)
        dxhat = dXn * gamma
        dx = rstd * (dxhat - jnp.mean(dxhat, axis=-1, keepdims=True) - xhat * jnp.mean(dxhat * xhat, axis=-1, keepdims=True))
        dX = (dY.astype(F32) + dx).astype(BF)
        return Y, dX, dW1, dW2, dgamma

    return jax.shard_map(block, mesh=mesh,
                         in_specs=(rows, P(None), P(None, "tp"), P("tp", None), rows),
                         out_specs=(rows, rows, P("data", "tp"), rows, P("data")),
                         check_vma=False)
```

```python
import functools
import math

import jax
import jax.numpy as jnp
from jax import lax
from jax.experimental import pallas as pl
from jax.experimental.pallas import tpu as pltpu
from jax.sharding import PartitionSpec as P


EPS = 1e-6
BF = jnp.bfloat16
F32 = jnp.float32


def _gelu(a):
    return jax.nn.gelu(a, approximate=True)


def _ln(x):
    mu = jnp.mean(x, axis=-1, keepdims=True)
    xc = x - mu
    var = jnp.mean(xc * xc, axis=-1, keepdims=True)
    rstd = lax.rsqrt(var + EPS)
    return xc * rstd, rstd


def _nn(a, b):
    return jnp.dot(a, b, preferred_element_type=F32)


def _tn(a, b):
    return lax.dot_general(a, b, (((0,), (0,)), ((), ())), preferred_element_type=F32)


def _nt(a, b):
    return lax.dot_general(a, b, (((1,), (1,)), ((), ())), preferred_element_type=F32)


def _swap(bit):
    return lambda v: lax.ppermute(v, "tp", [(i, i ^ bit) for i in range(8)])


CORE, XN, YN = _swap(1), _swap(2), _swap(4)


def ZN(v):
    return lax.ppermute(v, "data", [(0, 1), (1, 0)])


def _dact(A, dH):
    return jax.vjp(_gelu, A)[1](dH)[0].astype(BF)


def _cat(*v):
    return jnp.concatenate(v)


tie = lambda *v: lax.optimization_barrier(v)


ROWS = 512


def _mlp_kernel(steps, nw, acc, *refs):
    x_hbm, dy_hbm, w1s, w2s = refs[0], refs[1], refs[2:2 + nw], refs[2 + nw:2 + 2 * nw]
    refs = refs[2 + 2 * nw:]
    ins, refs = (refs[:4], refs[4:]) if acc else ((), refs)
    outs, (xb, yb, ya, da, w1b, w2b, wsem, xsem, asem, osem) = refs[:4], refs[4:]
    nb = len(steps)
    tiles = xb.shape[0] // ROWS
    width = xb.shape[1]

    def fetch(j, slot):
        at = 0
        for k, lo, r in steps[j]:
            pltpu.make_async_copy(w1s[k].at[:, pl.ds(lo, r)], w1b.at[slot, :, pl.ds(at, r)], wsem.at[0, slot]).start()
            pltpu.make_async_copy(w2s[k].at[pl.ds(lo, r)], w2b.at[slot, pl.ds(at, r)], wsem.at[1, slot]).start()
            at += r

    loads = [pltpu.make_async_copy(x_hbm, xb, xsem.at[0]), pltpu.make_async_copy(dy_hbm, yb, xsem.at[1])]
    sums = [(b, t) for b in (ya, da) for t in range(tiles)]
    fills = [pltpu.make_async_copy(r, b.at[pl.ds(t * ROWS, ROWS)], asem.at[i]) for i, (r, (b, t)) in enumerate(zip(ins, sums))]
    for c in loads:
        c.start()
    fetch(0, 0)
    for c in fills:
        c.start()
    if not acc:
        ya[...] = jnp.zeros_like(ya)
        da[...] = jnp.zeros_like(da)
    for c in loads:
        c.wait()
    for c in fills:
        c.wait()

    @pl.loop(0, nb)
    def _(j):
        slot = lax.rem(j, 2)
        pltpu.make_async_copy(w1b.at[slot], w1b.at[slot], wsem.at[0, slot]).wait()
        pltpu.make_async_copy(w2b.at[slot], w2b.at[slot], wsem.at[1, slot]).wait()
        for k in range(1, nb):
            @pl.when(j + 1 == k)
            def _():
                fetch(k, k % 2)

        @pl.loop(0, tiles)
        def _(t):
            m = pl.ds(pl.multiple_of(t * ROWS, ROWS), ROWS)
            a = jnp.dot(xb[m], w1b[slot], preferred_element_type=F32)
            dh = lax.dot_general(yb[m], w2b[slot], (((1,), (1,)), ((), ())), preferred_element_type=F32)
            c = math.sqrt(2 / math.pi)
            th = jnp.tanh(c * (a + 0.044715 * (a * a * a)))
            cdf = 0.5 * (1.0 + th)
            h = (a * cdf).astype(BF)
            d = (dh * (cdf + 0.5 * a * (1.0 - th * th) * (c * (1.0 + 3 * 0.044715 * (a * a))))).astype(BF)

            @pl.loop(0, width // ROWS)
            def _(i):
                n = pl.ds(pl.multiple_of(i * ROWS, ROWS), ROWS)
                ya[m, n] += jnp.dot(h, w2b[slot, :, n], preferred_element_type=F32)
                da[m, n] += lax.dot_general(d, w1b[slot, n], (((1,), (1,)), ((), ())), preferred_element_type=F32)

            for i, (b, tt) in enumerate(sums):
                @pl.when((j == nb - 1) & (t == tt))
                def _():
                    pltpu.make_async_copy(b.at[pl.ds(tt * ROWS, ROWS)], outs[i], osem.at[i]).start()

    for i, (b, tt) in enumerate(sums):
        pltpu.make_async_copy(b.at[pl.ds(tt * ROWS, ROWS)], outs[i], osem.at[i]).wait()


def mlp(x, dy, steps, w1s, w2s, sums=()):
    tokens, width = x.shape
    nw, nb = len(w1s), len(steps)
    hbm = pl.BlockSpec(memory_space=pl.ANY)
    return pl.pallas_call(
        functools.partial(_mlp_kernel, steps, nw, bool(sums)),
        out_shape=[jax.ShapeDtypeStruct((ROWS, width), F32)] * 4,
        in_specs=[hbm] * (2 + 2 * nw + len(sums)),
        out_specs=[hbm] * 4,
        scratch_shapes=[
            pltpu.VMEM((tokens, width), BF), pltpu.VMEM((tokens, width), BF),
            pltpu.VMEM((tokens, width), F32), pltpu.VMEM((tokens, width), F32),
            pltpu.VMEM((2, width, ROWS), BF), pltpu.VMEM((2, ROWS, width), BF),
            pltpu.SemaphoreType.DMA((2, 2)), pltpu.SemaphoreType.DMA((2,)),
            pltpu.SemaphoreType.DMA((4,)), pltpu.SemaphoreType.DMA((4,)),
        ],
        input_output_aliases={2 + 2 * nw + i: i for i in range(len(sums))},
        compiler_params=pltpu.CompilerParams(vmem_limit_bytes=63 * 1024 * 1024),
        cost_estimate=pl.CostEstimate(flops=8 * tokens * width * ROWS * nb, transcendentals=tokens * ROWS * nb,
                                      bytes_accessed=4 * width * ROWS * nb + 20 * tokens * width),
    )(x, dy, *w1s, *w2s, *sums)


def solution(mesh):
    rows = P(("data", "tp"), None)

    def block(X, gamma, W1, W2, dY):
        n = X.shape[0]
        zi = lax.axis_index("data")
        half = W2.shape[0] // 2
        q = half // 2

        def piece1(w, c):
            return lax.dynamic_slice_in_dim(w, zi * half + c * q, q, 1)

        def piece2(w, c):
            return lax.dynamic_slice_in_dim(w, zi * half + c * q, q, 0)

        Xp, dYp = CORE(X), CORE(dY)
        a1, a2 = piece1(W1, 0), piece2(W2, 0)
        x1, y1, x2, y2 = XN(a1), YN(a1), XN(a2), YN(a2)
        Xs, a1, a2 = tie(X, a1, a2)
        x = Xs.astype(F32)
        xhat, rstd = _ln(x)
        Xn = (xhat * gamma).astype(BF)
        m = n // 2
        gather = lambda v: lax.all_gather(v, "tp", axis=0, tiled=True)
        XaL, gL, XaH, gH = gather(Xn[:m]), gather(dY[:m]), gather(Xn[m:]), gather(dY[m:])
        W1s, W2s, Xn, Xp, dYp = tie(W1, W2, Xn, Xp, dYp)
        b1, b2 = piece1(W1s, 1), piece2(W2s, 1)
        bx1, by1, bx2, by2 = XN(b1), YN(b1), XN(b2), YN(b2)
        b1, b2, Xp = tie(b1, b2, Xp)
        Xnc = _cat(Xn, (_ln(Xp.astype(F32))[0] * gamma).astype(BF))
        dYc = _cat(dY, dYp)
        S = mlp(Xnc, dYc, [[(0, 0, ROWS)], [(0, ROWS, ROWS)]], [W1], [W2])
        x1, y1, x2, y2, *S = tie(x1, y1, x2, y2, *S)
        zx1, zy1, d1 = ZN(x1), ZN(y1), XN(y1)
        zx2, zy2, d2 = ZN(x2), ZN(y2), YN(x2)
        pair = lambda k: [(k, 0, q), (k + 1, 0, q)]
        S = mlp(Xnc, dYc, [pair(0)], [x1, y1], [x2, y2], S)
        XaL, *S = tie(XaL, *S)
        AL = _nn(XaL, W1)
        gL, bx1, by1, bx2, by2, AL = tie(gL, bx1, by1, bx2, by2, AL)
        bzx1, bzy1, bzx2, bzy2 = ZN(bx1), ZN(by1), ZN(bx2), ZN(by2)
        bd1, bd2 = XN(by1), YN(bx2)
        dAL = _dact(AL, _nt(gL, W2))
        d1, d2, dAL = tie(d1, d2, dAL)
        zd1, zd2 = ZN(d1), ZN(d2)
        dW2, dW1 = _tn(_gelu(AL).astype(BF), gL), _tn(XaL, dAL)
        zx1, zy1, zx2, zy2, dW2, dW1, *S = tie(zx1, zy1, zx2, zy2, dW2, dW1, *S)
        S = mlp(Xnc, dYc, [pair(0), pair(2)], [bx1, by1, zx1, zy1], [bx2, by2, zx2, zy2], S)
        XaH, bd1, bd2, *S = tie(XaH, bd1, bd2, *S)
        bzd1, bzd2 = ZN(bd1), ZN(bd2)
        AH = _nn(XaH, W1)
        gH, AH, dW2, dW1 = tie(gH, AH, dW2, dW1)
        dAH = _dact(AH, _nt(gH, W2))
        dW2, dW1 = dW2 + _tn(_gelu(AH).astype(BF), gH), dW1 + _tn(XaH, dAH)
        bzx1, bzy1, bzx2, bzy2, zd1, zd2, dW2, dW1, *S = tie(bzx1, bzy1, bzx2, bzy2, zd1, zd2, dW2, dW1, *S)
        S = mlp(Xnc, dYc, [pair(0), pair(2)], [bzx1, bzy1, d1, zd1], [bzx2, bzy2, d2, zd2], S)
        bzd1, bzd2, *S = tie(bzd1, bzd2, *S)
        Yo, Yp, dXo, dXp = mlp(Xnc, dYc, [pair(0)], [bd1, bzd1], [bd2, bzd2], S)

        dXn = dXo + CORE(dXp)
        Y = (x + (Yo + CORE(Yp))).astype(BF)
        dgamma = jnp.sum(dXn * xhat, axis=0)
        for hop in (CORE, XN, YN):
            dgamma = dgamma + hop(dgamma)
        dxhat = dXn * gamma
        dx = rstd * (dxhat - jnp.mean(dxhat, axis=-1, keepdims=True) - xhat * jnp.mean(dxhat * xhat, axis=-1, keepdims=True))
        dX = (dY.astype(F32) + dx).astype(BF)
        return Y, dX, dW1, dW2, dgamma

    return jax.shard_map(block, mesh=mesh,
                         in_specs=(rows, P(None), P(None, "tp"), P("tp", None), rows),
                         out_specs=(rows, rows, P("data", "tp"), rows, P("data")),
                         check_vma=False)
```
